32 devices in a mesh: fsdp: 16 (over z, y, x), dp: 2 (over core).
Axes of the slice: x: 2, y: 2, z: 4, core: 2. Of those that a mesh axis runs over, the one named last changes fastest.
Arguments:
- normed: bfloat16 [2, 4096, 4096], P(None, ('fsdp', 'dp')), may hold values from -6 to 6
- kv_cotangent: bfloat16 [2, 4096, 512], P(None, ('fsdp', 'dp')), may hold values from -6 to 6
- kv_weight: bfloat16 [4096, 512], P('fsdp'), may hold values from -0.09375 to 0.09375
- main_grad: float32 [4096, 512], P('fsdp'), may hold values from -6 to 6
- owner_order: int32 [16], replicated, may hold values from 0 to 15, each once
Outputs:
- key_rows: bfloat16 [2, 4096, 512], P(None, ('fsdp', 'dp'))
- input_grad: bfloat16 [2, 4096, 4096], P(None, ('fsdp', 'dp'))
- grad_buffer: float32 [4096, 512], P('fsdp')
The draws below stay inside these ranges and needn't reach their ends.
Inputs may be any that keep to these rules, and one draw needn't show every extreme that they name: `owner_order`: a permutation: each value appears once.
All inputs are finite; a program needn't handle non-finite values.
Results may differ from the reference program's by a relative error of at most 0.0075.
Values may be sent and summed in bfloat16 or wider, within the bound.
No kernel may reach another device: no remote copies, remote signals or barrier semaphores. Data moves between devices by JAX's collectives and lax.ppermute only.
A program may use at most 64 MiB of HBM per device.

```python
import math
import jax
import jax.numpy as jnp
from jax import lax

D = 4096
MICRO = 2
TOK_DEV = 128
KVW = 512
TOKENS = 4096
N_FSDP = 16
N_DP = 2


def steps_of(rng, dims, split, smallest, high):
    level = 1.0
    for axis_at, blocks in split:
        heights = jax.random.uniform(jax.random.fold_in(jax.random.fold_in(rng, 6), axis_at), (blocks,), jnp.float32, smallest / len(split), high / len(split))
        level = level * jnp.repeat(jnp.exp(heights), dims[axis_at] // blocks).reshape((-1,) + (1,) * (len(dims) - 1 - axis_at))
    return level


def gaussian(rng, shape, scale, reach, cuts=(), kind=jnp.bfloat16):
    level = steps_of(rng, shape, cuts, -0.22, 0.18) if cuts else 1.0
    array = jax.random.normal(rng, shape, jnp.float32) * scale * level
    return jnp.minimum(jnp.maximum(array, -reach), reach).astype(kind)


def setup_inputs(seed: int = 0) -> dict:
    key_list = jax.random.split(jax.random.key(seed), 6)
    normed = gaussian(key_list[0], (MICRO, TOKENS, D), 1.0, 6.0, ((1, 32),))
    kv_cotangent = gaussian(key_list[1], (MICRO, TOKENS, KVW), 1.0, 6.0, ((1, 32),))
    kv_weight = gaussian(key_list[2], (D, KVW), D ** -0.5, 0.09375, ((0, 16),))
    main_grad = gaussian(key_list[3], (D, KVW), 1.0, 6.0, ((0, 16),), jnp.float32)
    owner_order = jax.random.permutation(key_list[4], N_FSDP).astype(jnp.int32)
    return dict(normed=normed, kv_cotangent=kv_cotangent, kv_weight=kv_weight, main_grad=main_grad, owner_order=owner_order)


def reference(normed, kv_cotangent, kv_weight, main_grad, owner_order):
    shard_rows = D // N_FSDP
    block_count = MICRO * N_DP
    block_rows = TOK_DEV * N_FSDP
    inverse_owner = jnp.argsort(owner_order).astype(jnp.int32)
    blocks_in = normed.reshape(block_count, block_rows, D)
    blocks_cot = kv_cotangent.reshape(block_count, block_rows, KVW)

    def advance(grad_sum, inputs_pair):
        inputs, cotangent = inputs_pair
        permuted = inputs.reshape(block_rows, N_FSDP, shard_rows)[:, owner_order, :].reshape(block_rows, D)
        key_block = jnp.dot(permuted, kv_weight, preferred_element_type=jnp.float32).astype(jnp.bfloat16)
        grad_permuted = jnp.dot(cotangent, kv_weight.T, preferred_element_type=jnp.float32).astype(jnp.bfloat16)
        grad_block = grad_permuted.reshape(block_rows, N_FSDP, shard_rows)[:, inverse_owner, :].reshape(block_rows, D)
        grad_sum = grad_sum + jnp.dot(permuted.T, cotangent, preferred_element_type=jnp.float32)
        return (grad_sum, (key_block, grad_block))
    grad_sum, outputs = lax.scan(advance, jnp.zeros((D, KVW), jnp.float32), (blocks_in, blocks_cot))
    key_blocks, grad_blocks = outputs
    grad_scale = 1.0 / math.sqrt(MICRO * TOKENS)
    grad_buffer = main_grad + grad_sum * grad_scale
    return (key_blocks.reshape(MICRO, TOKENS, KVW), grad_blocks.reshape(MICRO, TOKENS, D), grad_buffer)
```

```python
import functools
import math

import jax
import jax.numpy as jnp
from jax import lax
from jax.experimental import pallas as pl
from jax.experimental.pallas import tpu as pltpu
from jax.sharding import PartitionSpec as P

LANES = 128


def plain_body(normed, kv_cotangent, kv_weight, main_grad, owner_order):
    micro_count, tok_dev, width = normed.shape
    shard_rows, key_width = kv_weight.shape
    owners = lax.axis_size("fsdp")
    everyone = owners * lax.axis_size("dp")
    all_rows = micro_count * tok_dev
    permuted = jnp.take(normed.reshape(all_rows, owners, shard_rows), owner_order, axis=1).reshape(
        all_rows, width
    )
    flat_cot = kv_cotangent.reshape(all_rows, key_width)
    gathered = lax.all_gather(kv_weight, "fsdp", axis=0, tiled=True)
    key_sum = jnp.dot(permuted, gathered, preferred_element_type=jnp.float32)
    grad_permuted = lax.dot_general(
        flat_cot, gathered, (((1,), (1,)), ((), ())), preferred_element_type=jnp.float32
    ).astype(jnp.bfloat16)
    inverse_owner = jnp.argsort(owner_order)
    input_grad = jnp.take(
        grad_permuted.reshape(all_rows, owners, shard_rows), inverse_owner, axis=1
    ).reshape(micro_count, tok_dev, width)
    partial = lax.dot_general(
        permuted, flat_cot, (((0,), (0,)), ((), ())), preferred_element_type=jnp.float32
    )
    shard_sum = lax.psum_scatter(partial, "fsdp", scatter_dimension=0, tiled=True)
    replica_total = lax.psum(shard_sum, "dp")
    grad_scale = 1.0 / math.sqrt(micro_count * tok_dev * everyone)
    grad_buffer = main_grad + replica_total * grad_scale
    key_rows = key_sum.astype(jnp.bfloat16).reshape(micro_count, tok_dev, key_width)
    return (key_rows, input_grad, grad_buffer)


def grid_of(mesh):
    count = mesh.shape["fsdp"]
    spots = [getattr(d, "coords", None) for d in mesh.devices.reshape(count, -1)[:, 0]]
    if any(s is None for s in spots):
        return None
    sizes, step = [], 1
    while step < count:
        axis = [i for i in range(3) if spots[step][i] != spots[0][i]]
        if len(axis) != 1:
            return None
        seen = 1
        while seen * step < count and all(
            spots[seen * step][i] == spots[0][i] for i in range(3) if i != axis[0]
        ):
            seen += 1
        sizes.insert(0, seen)
        step *= seen
    return tuple(sizes)


def pack_kernel(blocks, x_ref, cot_ref, out_ref):
    other = 1 - lax.axis_index("dp") % 2
    for g in range(blocks):
        start = pl.multiple_of((2 * g + other) * LANES, LANES)
        out_ref[:, g * LANES : (g + 1) * LANES] = x_ref[:, pl.ds(start, LANES)]
    out_ref[:, blocks * LANES :] = cot_ref[...]


def owner_at(grid, spot):
    nz, ny, nx = grid
    me = lax.axis_index("fsdp")
    z, y, x = me // (ny * nx), me // nx % ny, me % nx
    dz, dy, dx = spot
    return (((z + dz) % nz) * ny + (y + dy) % ny) * nx + (x + dx) % nx


def wgrad_kernel(grid, lists, order_ref, x_ref, cot_ref, got_ref, *outs):
    half = lax.axis_index("dp") % 2
    blocks = math.prod(grid)
    cot = jnp.concatenate([cot_ref[...], got_ref[:, blocks * LANES :]], axis=0)
    for out, spots in zip(outs, lists):
        columns = []
        for spot in spots:
            col = order_ref[owner_at(grid, spot)]
            own = x_ref[:, pl.ds(pl.multiple_of((2 * col + half) * LANES, LANES), LANES)]
            got = got_ref[:, pl.ds(pl.multiple_of(col * LANES, LANES), LANES)]
            columns.append(jnp.concatenate([own, got], axis=0))
        out[...] = lax.dot_general(
            jnp.concatenate(columns, axis=1),
            cot,
            (((0,), (0,)), ((), ())),
            preferred_element_type=jnp.float32,
        ).astype(out.dtype)


def apply_kernel(grid, lists, order_ref, x_ref, cot_ref, *refs):
    half = lax.axis_index("dp") % 2
    weights, (key_ref, grad_ref) = refs[:-2], refs[-2:]
    cot = cot_ref[...]
    total = None
    for place, weight_ref in enumerate(weights):
        side = half if place % 2 == 0 else 1 - half
        starts = []
        for spot in lists[place // 2]:
            col = order_ref[owner_at(grid, spot)]
            starts.append(pl.multiple_of((2 * col + side) * LANES, LANES))
        weight = weight_ref[...]
        columns = jnp.concatenate([x_ref[:, pl.ds(s, LANES)] for s in starts], axis=1)
        term = jnp.dot(columns, weight, preferred_element_type=jnp.float32)
        total = term if total is None else total + term
        back = lax.dot_general(
            cot, weight, (((1,), (1,)), ((), ())), preferred_element_type=jnp.float32
        ).astype(grad_ref.dtype)
        for k, s in enumerate(starts):
            grad_ref[:, pl.ds(s, LANES)] = back[:, k * LANES : (k + 1) * LANES]
    key_ref[...] = total.astype(key_ref.dtype)


def staged_body(grid, normed, kv_cotangent, kv_weight, main_grad, owner_order):
    nz, ny, nx = grid
    micro_count, tok_dev, width = normed.shape
    shard_rows, key_width = kv_weight.shape
    owners, replicas = lax.axis_size("fsdp"), lax.axis_size("dp")
    rows = micro_count * tok_dev
    part = shard_rows // 2
    half = lax.axis_index("dp") % 2
    f32, bf16 = jnp.float32, jnp.bfloat16
    vmem = pl.BlockSpec(memory_space=pltpu.VMEM)
    smem = pl.BlockSpec(memory_space=pltpu.SMEM)

    def send(value, move):
        pairs = []
        for z in range(nz):
            for y in range(ny):
                for x in range(nx):
                    for r in range(replicas):
                        tz, ty, tx, tr = move(z, y, x, r)
                        to = ((tz % nz) * ny + ty % ny) * nx + tx % nx
                        pairs.append((((z * ny + y) * nx + x) * replicas + r, to * replicas + tr))
        return lax.ppermute(value, ("fsdp", "dp"), pairs)

    over_x = functools.partial(send, move=lambda z, y, x, r: (z, y, x + 1, r))
    over_y = functools.partial(send, move=lambda z, y, x, r: (z, y + 1, x, r))
    to_core = functools.partial(send, move=lambda z, y, x, r: (z, y, x, r ^ 1))

    def over_z(value, far):
        return send(value, lambda z, y, x, r: (z + far, y, x, r))

    flat = normed.reshape(rows, width)
    cot = kv_cotangent.reshape(rows, key_width)

    chunk = rows // 4
    packed = pl.pallas_call(
        functools.partial(pack_kernel, owners),
        grid=(4,),
        in_specs=[
            pl.BlockSpec((chunk, width), lambda i: (i, 0)),
            pl.BlockSpec((chunk, key_width), lambda i: (i, 0)),
        ],
        out_specs=pl.BlockSpec((chunk, width // 2 + key_width), lambda i: (i, 0)),
        out_shape=jax.ShapeDtypeStruct((rows, width // 2 + key_width), bf16),
        name="pack",
    )(flat, cot)
    got = to_core(packed)

    own = lax.dynamic_slice_in_dim(kv_weight, half * part, part, axis=0)
    line = [own] + [over_z(own, far) for far in range(1, nz)]
    cut = nz // 2
    red = jnp.concatenate(line[:cut], axis=0)
    blue = jnp.concatenate(line[cut:], axis=0)
    red_x = over_x(red)
    blue_y = over_y(blue)
    red = jnp.concatenate([red, red_x], axis=0)
    blue = jnp.concatenate([blue, blue_y], axis=0)
    red_y = over_y(red)
    blue_x = over_x(blue)
    held = []
    for piece in (red, blue, red_y, blue_x):
        held += [piece, to_core(piece)]
    near, far = range(cut), range(cut, nz)
    piece_spots = [
        [(-k, 0, dx) for dx in (0, 1) for k in near],
        [(-k, dy, 0) for dy in (0, 1) for k in far],
        [(-k, 1, dx) for dx in (0, 1) for k in near],
        [(-k, dy, 1) for dy in (0, 1) for k in far],
    ]

    sums_spots = [
        [(k, 1, dx) for dx in (0, 1) for k in near],
        [(k, dy, 1) for dy in (0, 1) for k in far],
        [(k, 0, dx) for dx in (1, 0) for k in near],
        [(k, dy, 0) for dy in (1, 0) for k in far],
    ]
    shapes = [
        jax.ShapeDtypeStruct((part * len(s), key_width), t)
        for s, t in zip(sums_spots, (bf16, bf16, f32, f32))
    ]
    red_out, blue_out, red_keep, blue_keep = pl.pallas_call(
        functools.partial(wgrad_kernel, grid, sums_spots),
        in_specs=[smem, vmem, vmem, vmem],
        out_specs=[vmem] * 4,
        out_shape=shapes,
        cost_estimate=pl.CostEstimate(
            flops=2 * rows * width * key_width, bytes_accessed=8 * rows * width, transcendentals=0
        ),
        name="wgrad",
    )(owner_order, flat, cot, got)

    red_in = over_y(red_out)
    blue_in = over_x(blue_out)
    red_rows, blue_rows = part * len(near), part * len(far)
    red_far = (red_keep[:red_rows] + red_in[red_rows:]).astype(bf16)
    blue_far = (blue_keep[:blue_rows] + blue_in[blue_rows:]).astype(bf16)
    red_sum = red_keep[red_rows:] + red_in[:red_rows] + over_x(red_far)
    blue_sum = blue_keep[blue_rows:] + blue_in[:blue_rows] + over_y(blue_far)
    along = [red_sum[k * part : (k + 1) * part] for k in range(len(near))]
    along += [blue_sum[k * part : (k + 1) * part] for k in range(len(far))]
    total = along[0]
    for k in range(1, nz):
        total = total + over_z(along[k].astype(bf16), k)
    if replicas > 2:
        groups = [[r for r in range(replicas) if r % 2 == h] for h in (0, 1)]
        total = lax.psum(total, "dp", axis_index_groups=groups)
    grad_scale = 1.0 / math.sqrt(rows * owners * replicas)
    kept = lax.dynamic_slice_in_dim(main_grad, half * part, part, axis=0) + total * grad_scale
    there = to_core(kept)
    grad_buffer = jnp.where(
        half == 0,
        jnp.concatenate([kept, there], axis=0),
        jnp.concatenate([there, kept], axis=0),
    )

    key, input_grad = pl.pallas_call(
        functools.partial(apply_kernel, grid, piece_spots),
        in_specs=[smem, vmem, vmem] + [vmem] * len(held),
        out_specs=[vmem] * 2,
        out_shape=[
            jax.ShapeDtypeStruct((rows, key_width), bf16),
            jax.ShapeDtypeStruct((rows, width), bf16),
        ],
        cost_estimate=pl.CostEstimate(
            flops=4 * rows * width * key_width, bytes_accessed=8 * rows * width, transcendentals=0
        ),
        name="apply",
    )(owner_order, flat, cot, *held)
    return (
        key.reshape(micro_count, tok_dev, key_width),
        input_grad.reshape(micro_count, tok_dev, width),
        grad_buffer,
    )


def solution(mesh):
    in_specs = (
        P(None, ("fsdp", "dp"), None),
        P(None, ("fsdp", "dp"), None),
        P("fsdp", None),
        P("fsdp", None),
        P(),
    )
    out_specs = (P(None, ("fsdp", "dp"), None), P(None, ("fsdp", "dp"), None), P("fsdp", None))
    grid = grid_of(mesh)
    staged = grid is not None and len(grid) == 3 and grid[1:] == (2, 2)
    staged = staged and mesh.shape["dp"] % 2 == 0

    def body(normed, kv_cotangent, kv_weight, main_grad, owner_order):
        args = (normed, kv_cotangent, kv_weight, main_grad, owner_order)
        if staged and kv_weight.shape[0] == 2 * LANES:
            return staged_body(grid, *args)
        return plain_body(*args)

    return jax.shard_map(body, mesh=mesh, in_specs=in_specs, out_specs=out_specs, check_vma=False)
```

```python
import functools
import math

import jax
import jax.numpy as jnp
from jax import lax
from jax.experimental import pallas as pl
from jax.experimental.pallas import tpu as pltpu
from jax.sharding import PartitionSpec as P


LANES = 128


def plain_body(normed, kv_cotangent, kv_weight, main_grad, owner_order):
    micro_count, tok_dev, width = normed.shape
    shard_rows, key_width = kv_weight.shape
    owners = lax.axis_size("fsdp")
    everyone = owners * lax.axis_size("dp")
    all_rows = micro_count * tok_dev
    permuted = jnp.take(normed.reshape(all_rows, owners, shard_rows), owner_order, axis=1).reshape(
        all_rows, width
    )
    flat_cot = kv_cotangent.reshape(all_rows, key_width)
    gathered = lax.all_gather(kv_weight, "fsdp", axis=0, tiled=True)
    key_sum = jnp.dot(permuted, gathered, preferred_element_type=jnp.float32)
    grad_permuted = lax.dot_general(
        flat_cot, gathered, (((1,), (1,)), ((), ())), preferred_element_type=jnp.float32
    ).astype(jnp.bfloat16)
    inverse_owner = jnp.argsort(owner_order)
    input_grad = jnp.take(
        grad_permuted.reshape(all_rows, owners, shard_rows), inverse_owner, axis=1
    ).reshape(micro_count, tok_dev, width)
    partial = lax.dot_general(
        permuted, flat_cot, (((0,), (0,)), ((), ())), preferred_element_type=jnp.float32
    )
    shard_sum = lax.psum_scatter(partial, "fsdp", scatter_dimension=0, tiled=True)
    replica_total = lax.psum(shard_sum, "dp")
    grad_scale = 1.0 / math.sqrt(micro_count * tok_dev * everyone)
    grad_buffer = main_grad + replica_total * grad_scale
    key_rows = key_sum.astype(jnp.bfloat16).reshape(micro_count, tok_dev, key_width)
    return (key_rows, input_grad, grad_buffer)


def grid_of(mesh):
    count = mesh.shape["fsdp"]
    spots = [getattr(d, "coords", None) for d in mesh.devices.reshape(count, -1)[:, 0]]
    if any(s is None for s in spots):
        return None
    sizes, step = [], 1
    while step < count:
        axis = [i for i in range(3) if spots[step][i] != spots[0][i]]
        if len(axis) != 1:
            return None
        seen = 1
        while seen * step < count and all(
            spots[seen * step][i] == spots[0][i] for i in range(3) if i != axis[0]
        ):
            seen += 1
        sizes.insert(0, seen)
        step *= seen
    return tuple(sizes)


def owner_at(grid, spot):
    nz, ny, nx = grid
    me = lax.axis_index("fsdp")
    z, y, x = me // (ny * nx), me // nx % ny, me % nx
    dz, dy, dx = spot
    return (((z + dz) % nz) * ny + (y + dy) % ny) * nx + (x + dx) % nx


def wgrad_kernel(grid, lists, order_ref, x_ref, cot_ref, xgot_ref, cgot_ref, *outs):
    half = lax.axis_index("dp") % 2
    cot = jnp.concatenate([cot_ref[...], cgot_ref[...]], axis=0)
    for out, spots in zip(outs, lists):
        columns = []
        for spot in spots:
            col = order_ref[owner_at(grid, spot)]
            at = pl.ds(pl.multiple_of((2 * col + half) * LANES, LANES), LANES)
            columns.append(jnp.concatenate([x_ref[:, at], xgot_ref[:, at]], axis=0))
        out[...] = lax.dot_general(
            jnp.concatenate(columns, axis=1),
            cot,
            (((0,), (0,)), ((), ())),
            preferred_element_type=jnp.float32,
        ).astype(out.dtype)


def apply_kernel(grid, pieces, first, order_ref, x_ref, cot_ref, *refs):
    half = lax.axis_index("dp") % 2
    refs = list(refs)
    scratch, sems = refs[-2:]
    key_ref, grad_ref = refs[-4:-2]
    weights = refs[: len(pieces)]
    cot = cot_ref[...]
    total = None if first else refs[len(pieces)][...]
    copies = []
    for place, (weight_ref, (spots, partner)) in enumerate(zip(weights, pieces)):
        side = 1 - half if partner else half
        starts = []
        for spot in spots:
            col = order_ref[owner_at(grid, spot)]
            starts.append(pl.multiple_of((2 * col + side) * LANES, LANES))
        weight = weight_ref[...]
        back = lax.dot_general(
            cot, weight, (((1,), (1,)), ((), ())), preferred_element_type=jnp.float32
        )
        scratch[place] = back.astype(scratch.dtype)
        for k, s in enumerate(starts):
            copy = pltpu.make_async_copy(
                scratch.at[place, :, k * LANES : (k + 1) * LANES],
                grad_ref.at[:, pl.ds(s, LANES)],
                sems.at[len(copies)],
            )
            copy.start()
            copies.append(copy)
        columns = jnp.concatenate([x_ref[:, pl.ds(s, LANES)] for s in starts], axis=1)
        term = jnp.dot(columns, weight, preferred_element_type=jnp.float32)
        total = term if total is None else total + term
    key_ref[...] = total.astype(key_ref.dtype)
    for copy in copies:
        copy.wait()


def staged_body(grid, normed, kv_cotangent, kv_weight, main_grad, owner_order):
    nz, ny, nx = grid
    micro_count, tok_dev, width = normed.shape
    shard_rows, key_width = kv_weight.shape
    owners, replicas = lax.axis_size("fsdp"), lax.axis_size("dp")
    rows = micro_count * tok_dev
    part = shard_rows // 2
    half = lax.axis_index("dp") % 2
    f32, bf16 = jnp.float32, jnp.bfloat16
    vmem = pl.BlockSpec(memory_space=pltpu.VMEM)
    smem = pl.BlockSpec(memory_space=pltpu.SMEM)
    anywhere = pl.BlockSpec(memory_space=pl.ANY)

    def send(value, move):
        pairs = []
        for z in range(nz):
            for y in range(ny):
                for x in range(nx):
                    for r in range(replicas):
                        tz, ty, tx, tr = move(z, y, x, r)
                        to = ((tz % nz) * ny + ty % ny) * nx + tx % nx
                        pairs.append((((z * ny + y) * nx + x) * replicas + r, to * replicas + tr))
        return lax.ppermute(value, ("fsdp", "dp"), pairs)

    def over_x(value):
        return send(value, lambda z, y, x, r: (z, y, x + 1, r))

    def over_y(value):
        return send(value, lambda z, y, x, r: (z, y + 1, x, r))

    def over_z(value, far):
        return send(value, lambda z, y, x, r: (z + far, y, x, r))

    def to_core(value):
        return send(value, lambda z, y, x, r: (z, y, x, r ^ 1))

    flat = normed.reshape(rows, width)
    cot = kv_cotangent.reshape(rows, key_width)
    cut = nz // 2
    near, far = range(cut), range(cut, nz)
    red_rows, blue_rows = part * len(near), part * len(far)

    xgot = to_core(flat)
    cgot = to_core(cot)

    def wgrad(lists, dtype):
        return pl.pallas_call(
            functools.partial(wgrad_kernel, grid, lists),
            in_specs=[smem] + [vmem] * 4,
            out_specs=[vmem] * len(lists),
            out_shape=[
                jax.ShapeDtypeStruct((part * len(s), key_width), dtype) for s in lists
            ],
            cost_estimate=pl.CostEstimate(
                flops=rows * width * key_width,
                bytes_accessed=4 * rows * width,
                transcendentals=0,
            ),
            compiler_params=pltpu.CompilerParams(vmem_limit_bytes=24 << 20),
        )(owner_order, flat, cot, xgot, cgot)

    red_out, blue_out = wgrad(
        [
            [(k, 1, dx) for dx in (0, 1) for k in near],
            [(k, dy, 1) for dy in (0, 1) for k in far],
        ],
        bf16,
    )
    red_on, blue_on, red_keep, blue_keep = wgrad(
        [
            [(k, 0, 1) for k in near],
            [(k, 1, 0) for k in far],
            [(k, 0, 0) for k in near],
            [(k, 0, 0) for k in far],
        ],
        f32,
    )

    own = lax.dynamic_slice_in_dim(kv_weight, half * part, part, axis=0)
    line = [own] + [over_z(own, d) for d in range(1, nz)]
    red = jnp.concatenate(line[:cut], axis=0)
    blue = jnp.concatenate(line[cut:], axis=0)
    red = jnp.concatenate([red, over_x(red)], axis=0)
    blue = jnp.concatenate([blue, over_y(blue)], axis=0)
    red_y = over_y(red)
    blue_x = over_x(blue)
    red_spots = [(-k, 0, dx) for dx in (0, 1) for k in near]
    blue_spots = [(-k, dy, 0) for dy in (0, 1) for k in far]
    red_y_spots = [(-k, 1, dx) for dx in (0, 1) for k in near]
    blue_x_spots = [(-k, dy, 1) for dy in (0, 1) for k in far]

    red_in = over_y(red_out)
    blue_in = over_x(blue_out)
    red_far = (red_on + red_in[red_rows:]).astype(bf16)
    blue_far = (blue_on + blue_in[blue_rows:]).astype(bf16)
    red_sum = red_keep + red_in[:red_rows] + over_x(red_far)
    blue_sum = blue_keep + blue_in[:blue_rows] + over_y(blue_far)
    along = [red_sum[k * part : (k + 1) * part] for k in range(len(near))]
    along += [blue_sum[k * part : (k + 1) * part] for k in range(len(far))]
    total = along[0]
    for d in range(1, nz):
        total = total + over_z(along[d].astype(bf16), d)
    if replicas > 2:
        groups = [[r for r in range(replicas) if r % 2 == h] for h in (0, 1)]
        total = lax.psum(total, "dp", axis_index_groups=groups)
    grad_scale = 1.0 / math.sqrt(rows * owners * replicas)
    kept = lax.dynamic_slice_in_dim(main_grad, half * part, part, axis=0) + total * grad_scale
    there = to_core(kept)
    grad_buffer = jnp.where(
        half == 0,
        jnp.concatenate([kept, there], axis=0),
        jnp.concatenate([there, kept], axis=0),
    )

    def apply(pieces, before, last):
        weights = [w for w, _, _ in pieces]
        inputs = [owner_order, flat, cot, *weights, *before]
        specs = [smem, vmem, vmem] + [vmem] * len(pieces) + [vmem, anywhere][: len(before)]
        return pl.pallas_call(
            functools.partial(apply_kernel, grid, [p[1:] for p in pieces], not before),
            in_specs=specs,
            out_specs=[vmem, anywhere],
            out_shape=[
                jax.ShapeDtypeStruct((rows, key_width), bf16 if last else f32),
                jax.ShapeDtypeStruct((rows, width), bf16),
            ],
            scratch_shapes=[
                pltpu.VMEM((len(pieces), rows, max(w.shape[0] for w in weights)), bf16),
                pltpu.SemaphoreType.DMA((sum(len(p[1]) for p in pieces),)),
            ],
            input_output_aliases={len(inputs) - 1: 1} if before else {},
            cost_estimate=pl.CostEstimate(
                flops=4 * rows * key_width * sum(w.shape[0] for w in weights),
                bytes_accessed=2 * rows * width,
                transcendentals=0,
            ),
            compiler_params=pltpu.CompilerParams(vmem_limit_bytes=24 << 20),
        )(*inputs)

    done = apply(
        [
            (red, red_spots, False),
            (blue, blue_spots, False),
            (to_core(red), red_spots, True),
            (to_core(blue), blue_spots, True),
        ],
        (),
        False,
    )
    done = apply([(red_y, red_y_spots, False), (blue_x, blue_x_spots, False)], done, False)
    key, input_grad = apply(
        [(to_core(red_y), red_y_spots, True), (to_core(blue_x), blue_x_spots, True)], done, True
    )
    return (
        key.reshape(micro_count, tok_dev, key_width),
        input_grad.reshape(micro_count, tok_dev, width),
        grad_buffer,
    )


def solution(mesh):
    in_specs = (
        P(None, ("fsdp", "dp"), None),
        P(None, ("fsdp", "dp"), None),
        P("fsdp", None),
        P("fsdp", None),
        P(),
    )
    out_specs = (P(None, ("fsdp", "dp"), None), P(None, ("fsdp", "dp"), None), P("fsdp", None))
    grid = grid_of(mesh)
    staged = grid is not None and len(grid) == 3 and grid[1:] == (2, 2)
    staged = staged and mesh.shape["dp"] % 2 == 0

    def body(normed, kv_cotangent, kv_weight, main_grad, owner_order):
        args = (normed, kv_cotangent, kv_weight, main_grad, owner_order)
        if staged and kv_weight.shape[0] == 2 * LANES:
            return staged_body(grid, *args)
        return plain_body(*args)

    return jax.shard_map(body, mesh=mesh, in_specs=in_specs, out_specs=out_specs, check_vma=False)
```

```python
import functools
import math

import jax
import jax.numpy as jnp
from jax import lax
from jax.experimental import pallas as pl
from jax.experimental.pallas import tpu as pltpu
from jax.sharding import PartitionSpec as P


LANES = 128
TIGHT_BYTES = 62 << 20


def plain_body(normed, kv_cotangent, kv_weight, main_grad, owner_order):
    micro_count, tok_dev, width = normed.shape
    shard_rows, key_width = kv_weight.shape
    owners = lax.axis_size("fsdp")
    everyone = owners * lax.axis_size("dp")
    all_rows = micro_count * tok_dev
    permuted = jnp.take(normed.reshape(all_rows, owners, shard_rows), owner_order, axis=1).reshape(
        all_rows, width
    )
    flat_cot = kv_cotangent.reshape(all_rows, key_width)
    gathered = lax.all_gather(kv_weight, "fsdp", axis=0, tiled=True)
    key_sum = jnp.dot(permuted, gathered, preferred_element_type=jnp.float32)
    grad_permuted = lax.dot_general(
        flat_cot, gathered, (((1,), (1,)), ((), ())), preferred_element_type=jnp.float32
    ).astype(jnp.bfloat16)
    inverse_owner = jnp.argsort(owner_order)
    input_grad = jnp.take(
        grad_permuted.reshape(all_rows, owners, shard_rows), inverse_owner, axis=1
    ).reshape(micro_count, tok_dev, width)
    partial = lax.dot_general(
        permuted, flat_cot, (((0,), (0,)), ((), ())), preferred_element_type=jnp.float32
    )
    shard_sum = lax.psum_scatter(partial, "fsdp", scatter_dimension=0, tiled=True)
    replica_total = lax.psum(shard_sum, "dp")
    grad_scale = 1.0 / math.sqrt(micro_count * tok_dev * everyone)
    grad_buffer = main_grad + replica_total * grad_scale
    key_rows = key_sum.astype(jnp.bfloat16).reshape(micro_count, tok_dev, key_width)
    return (key_rows, input_grad, grad_buffer)


def grid_of(mesh):
    count = mesh.shape["fsdp"]
    spots = [getattr(d, "coords", None) for d in mesh.devices.reshape(count, -1)[:, 0]]
    if any(s is None for s in spots):
        return None
    sizes, step = [], 1
    while step < count:
        axis = [i for i in range(3) if spots[step][i] != spots[0][i]]
        if len(axis) != 1:
            return None
        seen = 1
        while seen * step < count and all(
            spots[seen * step][i] == spots[0][i] for i in range(3) if i != axis[0]
        ):
            seen += 1
        sizes.insert(0, seen)
        step *= seen
    return tuple(sizes)


def owner_at(grid, spot):
    nz, ny, nx = grid
    me = lax.axis_index("fsdp")
    z, y, x = me // (ny * nx), me // nx % ny, me % nx
    dz, dy, dx = spot
    return (((z + dz) % nz) * ny + (y + dy) % ny) * nx + (x + dx) % nx


def stage_kernel(grid, lists, order_ref, x_ref, cot_ref, *refs):
    outs, (buf, x_sems, cot_sems) = refs[: 2 * len(lists)], refs[2 * len(lists) :]
    chunks, step, _ = buf.shape
    half = lax.axis_index("dp") % 2
    loads = []
    for c in range(chunks):
        rows = pl.ds(c * step, step)
        loads.append(pltpu.make_async_copy(x_ref.at[rows], buf.at[c], x_sems.at[c]))
        loads[-1].start()
    stores = []
    for side in range(2):
        to_ref = outs[side * len(lists)]
        to = to_ref.at[:, len(lists[0]) * LANES :]
        stores.append(pltpu.make_async_copy(cot_ref, to, cot_sems.at[side]))
        stores[-1].start()
    starts = []
    for spots in lists:
        cols = [order_ref[owner_at(grid, spot)] for spot in spots]
        starts.append(cols)
    for c in range(chunks):
        loads[c].wait()
        rows = slice(c * step, (c + 1) * step)
        for side in range(2):
            which = half if side == 0 else 1 - half
            for cols, to_ref in zip(starts, outs[side * len(lists) :]):
                for k, col in enumerate(cols):
                    at = pl.ds(pl.multiple_of((2 * col + which) * LANES, LANES), LANES)
                    to_ref[rows, k * LANES : (k + 1) * LANES] = buf[c, :, at]
    for store in stores:
        store.wait()


def wgrad_kernel(cot_at, keep, *refs):
    first, refs = refs[:2], refs[2:]
    cot = jnp.concatenate([r[:, cot_at:] for r in first], axis=0)
    sources = first
    if keep:
        sources, refs = refs[:2], refs[2:]
    begin = 0
    for out in refs:
        at = slice(begin, begin + out.shape[0])
        out[...] = lax.dot_general(
            jnp.concatenate([r[:, at] for r in sources], axis=0),
            cot,
            (((0,), (0,)), ((), ())),
            preferred_element_type=jnp.float32,
        ).astype(out.dtype)
        begin += out.shape[0]


def apply_kernel(grid, pieces, first, last, order_ref, cot_ref, *refs):
    half = lax.axis_index("dp") % 2
    refs = list(refs)
    weights = [refs.pop(0) for _ in pieces]
    columns = {}
    for _, partner in pieces:
        if partner not in columns:
            columns[partner] = [refs.pop(0), 0]
    before_ref = None if first else refs.pop(0)
    if not first:
        refs.pop(0)
    halves = [refs.pop(0) for _ in range(2)] if last else []
    key_ref, grad_ref = refs.pop(0), refs.pop(0)
    buffer_ref = refs.pop(0) if last else None
    scratch, total_buf, key_buf, out_sems, sems = refs
    if not first:
        fetch = pltpu.make_async_copy(before_ref, total_buf, sems.at[0])
        fetch.start()
    stores = []
    for k, ref in enumerate(halves):
        part = ref.shape[0]
        side = half if k == 0 else 1 - half
        stores.append(
            pltpu.make_async_copy(
                ref, buffer_ref.at[pl.ds(pl.multiple_of(side * part, part), part)], sems.at[2 + k]
            )
        )
        stores[-1].start()
    cot = cot_ref[...]
    count = 0
    for place, (spots, partner) in enumerate(pieces):
        side = 1 - half if partner else half
        back = lax.dot_general(
            cot, weights[place][...], (((1,), (1,)), ((), ())), preferred_element_type=jnp.float32
        )
        scratch[place] = back.astype(scratch.dtype)
        for k, spot in enumerate(spots):
            col = order_ref[owner_at(grid, spot)]
            start = pl.multiple_of((2 * col + side) * LANES, LANES)
            stores.append(
                pltpu.make_async_copy(
                    scratch.at[place, :, k * LANES : (k + 1) * LANES],
                    grad_ref.at[:, pl.ds(start, LANES)],
                    out_sems.at[count],
                )
            )
            stores[-1].start()
            count += 1
    total = None
    for place, (spots, partner) in enumerate(pieces):
        source, begin = columns[partner]
        columns[partner][1] = end = begin + len(spots) * LANES
        term = jnp.dot(
            source[:, begin:end], weights[place][...], preferred_element_type=jnp.float32
        )
        total = term if total is None else total + term
    if not first:
        fetch.wait()
        total = total + total_buf[...]
    key_buf[...] = total.astype(key_buf.dtype)
    stores.append(pltpu.make_async_copy(key_buf, key_ref, sems.at[1]))
    stores[-1].start()
    for store in stores:
        store.wait()


def staged_body(grid, normed, kv_cotangent, kv_weight, main_grad, owner_order):
    nz, ny, nx = grid
    micro_count, tok_dev, width = normed.shape
    shard_rows, key_width = kv_weight.shape
    owners, replicas = lax.axis_size("fsdp"), lax.axis_size("dp")
    rows = micro_count * tok_dev
    part = shard_rows // 2
    half = lax.axis_index("dp") % 2
    f32, bf16 = jnp.float32, jnp.bfloat16
    vmem = pl.BlockSpec(memory_space=pltpu.VMEM)
    smem = pl.BlockSpec(memory_space=pltpu.SMEM)
    hbm = pl.BlockSpec(memory_space=pltpu.HBM)

    def send(value, move):
        pairs = []
        for z in range(nz):
            for y in range(ny):
                for x in range(nx):
                    for r in range(replicas):
                        tz, ty, tx, tr = move(z, y, x, r)
                        to = ((tz % nz) * ny + ty % ny) * nx + tx % nx
                        pairs.append((((z * ny + y) * nx + x) * replicas + r, to * replicas + tr))
        return lax.ppermute(value, ("fsdp", "dp"), pairs)

    def over_x(value):
        return send(value, lambda z, y, x, r: (z, y, x + 1, r))

    def over_y(value):
        return send(value, lambda z, y, x, r: (z, y + 1, x, r))

    def over_z(value, far):
        return send(value, lambda z, y, x, r: (z + far, y, x, r))

    def to_core(value):
        return send(value, lambda z, y, x, r: (z, y, x, r ^ 1))

    flat = normed.reshape(rows, width)
    cot = kv_cotangent.reshape(rows, key_width)
    cut = nz // 2
    near, far = range(cut), range(cut, nz)
    red_rows, blue_rows = part * len(near), part * len(far)

    far_spots = [(k, 1, dx) for dx in (0, 1) for k in near]
    far_spots += [(k, dy, 1) for dy in (0, 1) for k in far]
    near_spots = [(k, 0, dx) for dx in (0, 1) for k in near]
    near_spots += [(k, dy, 0) for dy in (0, 1) for k in far]
    far_wide, near_wide = part * len(far_spots), part * len(near_spots)
    shapes = [
        jax.ShapeDtypeStruct((rows, far_wide + key_width), bf16),
        jax.ShapeDtypeStruct((rows, near_wide), bf16),
    ]
    chunks = 4
    far_own, near_own, far_partner, near_partner = pl.pallas_call(
        functools.partial(stage_kernel, grid, [far_spots, near_spots]),
        in_specs=[smem, hbm, hbm],
        out_specs=[vmem] * 4,
        out_shape=shapes * 2,
        scratch_shapes=[
            pltpu.VMEM((chunks, rows // chunks, width), bf16),
            pltpu.SemaphoreType.DMA((chunks,)),
            pltpu.SemaphoreType.DMA((2,)),
        ],
        compiler_params=pltpu.CompilerParams(vmem_limit_bytes=TIGHT_BYTES),
        name="stage",
    )(owner_order, flat, cot)
    far_got = to_core(far_partner)
    near_got = to_core(near_partner)

    def wgrad(sources, sizes, dtype):
        return pl.pallas_call(
            functools.partial(wgrad_kernel, far_wide, len(sources) > 2),
            in_specs=[vmem] * len(sources),
            out_specs=[vmem] * len(sizes),
            out_shape=[jax.ShapeDtypeStruct((size, key_width), dtype) for size in sizes],
            cost_estimate=pl.CostEstimate(
                flops=rows * width * key_width,
                bytes_accessed=4 * rows * width,
                transcendentals=0,
            ),
            compiler_params=pltpu.CompilerParams(vmem_limit_bytes=24 << 20),
        )(*sources)

    red_out, blue_out = wgrad([far_own, far_got], [2 * red_rows, 2 * blue_rows], bf16)
    red_keep, red_on, blue_keep, blue_on = wgrad(
        [far_own, far_got, near_own, near_got], [red_rows, red_rows, blue_rows, blue_rows], f32
    )

    own = lax.dynamic_slice_in_dim(kv_weight, half * part, part, axis=0)
    line = [own] + [over_z(own, -d) for d in range(1, nz)]
    red = jnp.concatenate(line[:cut], axis=0)
    blue = jnp.concatenate(line[cut:], axis=0)
    red = jnp.concatenate([red, over_x(red)], axis=0)
    blue = jnp.concatenate([blue, over_y(blue)], axis=0)
    red_y = over_y(red)
    blue_x = over_x(blue)
    red_spots, blue_spots = near_spots[: 2 * len(near)], near_spots[2 * len(near) :]
    red_y_spots, blue_x_spots = far_spots[: 2 * len(near)], far_spots[2 * len(near) :]

    red_in = over_y(red_out)
    blue_in = over_x(blue_out)
    red_far = (red_on + red_in[red_rows:]).astype(bf16)
    blue_far = (blue_on + blue_in[blue_rows:]).astype(bf16)
    red_sum = red_keep + red_in[:red_rows] + over_x(red_far)
    blue_sum = blue_keep + blue_in[:blue_rows] + over_y(blue_far)
    along = [red_sum[k * part : (k + 1) * part] for k in range(len(near))]
    along += [blue_sum[k * part : (k + 1) * part] for k in range(len(far))]
    total = along[0]
    for d in range(1, nz):
        total = total + over_z(along[d].astype(bf16), d)
    if replicas > 2:
        groups = [[r for r in range(replicas) if r % 2 == h] for h in (0, 1)]
        total = lax.psum(total, "dp", axis_index_groups=groups)
    grad_scale = 1.0 / math.sqrt(rows * owners * replicas)
    kept = lax.dynamic_slice_in_dim(main_grad, half * part, part, axis=0) + total * grad_scale
    there = to_core(kept)

    def apply(pieces, columns, before, halves):
        weights = [w for w, _, _ in pieces]
        inputs = [owner_order, cot, *weights, *columns, *before, *halves]
        specs = [smem] + [vmem] * (1 + len(pieces) + len(columns)) + [hbm, hbm][: len(before)]
        specs += [vmem] * len(halves)
        count = sum(len(spots) for _, spots, _ in pieces)
        wide = max(w.shape[0] for w in weights)
        key_type = bf16 if halves else f32
        shapes = [
            jax.ShapeDtypeStruct((rows, key_width), key_type),
            jax.ShapeDtypeStruct((rows, width), bf16),
        ]
        if halves:
            shapes.append(jax.ShapeDtypeStruct((shard_rows, key_width), f32))
        return pl.pallas_call(
            functools.partial(
                apply_kernel, grid, [p[1:] for p in pieces], not before, bool(halves)
            ),
            in_specs=specs,
            out_specs=[hbm] * len(shapes),
            out_shape=shapes,
            scratch_shapes=[
                pltpu.VMEM((len(pieces), rows, wide), bf16),
                pltpu.VMEM((rows, key_width), f32),
                pltpu.VMEM((rows, key_width), key_type),
                pltpu.SemaphoreType.DMA((count,)),
                pltpu.SemaphoreType.DMA((4,)),
            ],
            input_output_aliases={len(inputs) - 1 - len(halves): 1} if before else {},
            cost_estimate=pl.CostEstimate(
                flops=4 * rows * key_width * sum(w.shape[0] for w in weights),
                bytes_accessed=2 * rows * width,
                transcendentals=0,
            ),
            compiler_params=pltpu.CompilerParams(vmem_limit_bytes=24 << 20),
        )(*inputs)

    done = apply(
        [
            (red, red_spots, False),
            (blue, blue_spots, False),
            (to_core(red), red_spots, True),
            (to_core(blue), blue_spots, True),
        ],
        [near_own, near_partner],
        (),
        (),
    )
    done = apply([(red_y, red_y_spots, False), (blue_x, blue_x_spots, False)], [far_own], done, ())
    key, input_grad, grad_buffer = apply(
        [(to_core(red_y), red_y_spots, True), (to_core(blue_x), blue_x_spots, True)],
        [far_partner],
        done,
        (kept, there),
    )
    return (
        key.reshape(micro_count, tok_dev, key_width),
        input_grad.reshape(micro_count, tok_dev, width),
        grad_buffer,
    )


def solution(mesh):
    in_specs = (
        P(None, ("fsdp", "dp"), None),
        P(None, ("fsdp", "dp"), None),
        P("fsdp", None),
        P("fsdp", None),
        P(),
    )
    out_specs = (P(None, ("fsdp", "dp"), None), P(None, ("fsdp", "dp"), None), P("fsdp", None))
    grid = grid_of(mesh)
    staged = grid is not None and len(grid) == 3 and grid[1:] == (2, 2)
    staged = staged and mesh.shape["dp"] % 2 == 0

    def body(normed, kv_cotangent, kv_weight, main_grad, owner_order):
        args = (normed, kv_cotangent, kv_weight, main_grad, owner_order)
        if staged and kv_weight.shape[0] == 2 * LANES:
            return staged_body(grid, *args)
        return plain_body(*args)

    return jax.shard_map(body, mesh=mesh, in_specs=in_specs, out_specs=out_specs, check_vma=False)
```

```python
import functools
import math

import jax
import jax.numpy as jnp
from jax import lax
from jax.experimental import pallas as pl
from jax.experimental.pallas import tpu as pltpu
from jax.sharding import PartitionSpec as P


LANES = 128
TIGHT_BYTES = (62 << 20) + (16 << 10)


def plain_body(normed, kv_cotangent, kv_weight, main_grad, owner_order):
    micro_count, tok_dev, width = normed.shape
    shard_rows, key_width = kv_weight.shape
    owners = lax.axis_size("fsdp")
    everyone = owners * lax.axis_size("dp")
    all_rows = micro_count * tok_dev
    permuted = jnp.take(normed.reshape(all_rows, owners, shard_rows), owner_order, axis=1).reshape(
        all_rows, width
    )
    flat_cot = kv_cotangent.reshape(all_rows, key_width)
    gathered = lax.all_gather(kv_weight, "fsdp", axis=0, tiled=True)
    key_sum = jnp.dot(permuted, gathered, preferred_element_type=jnp.float32)
    grad_permuted = lax.dot_general(
        flat_cot, gathered, (((1,), (1,)), ((), ())), preferred_element_type=jnp.float32
    ).astype(jnp.bfloat16)
    inverse_owner = jnp.argsort(owner_order)
    input_grad = jnp.take(
        grad_permuted.reshape(all_rows, owners, shard_rows), inverse_owner, axis=1
    ).reshape(micro_count, tok_dev, width)
    partial = lax.dot_general(
        permuted, flat_cot, (((0,), (0,)), ((), ())), preferred_element_type=jnp.float32
    )
    shard_sum = lax.psum_scatter(partial, "fsdp", scatter_dimension=0, tiled=True)
    replica_total = lax.psum(shard_sum, "dp")
    grad_scale = 1.0 / math.sqrt(micro_count * tok_dev * everyone)
    grad_buffer = main_grad + replica_total * grad_scale
    key_rows = key_sum.astype(jnp.bfloat16).reshape(micro_count, tok_dev, key_width)
    return (key_rows, input_grad, grad_buffer)


def grid_of(mesh):
    count = mesh.shape["fsdp"]
    spots = [getattr(d, "coords", None) for d in mesh.devices.reshape(count, -1)[:, 0]]
    if any(s is None for s in spots):
        return None
    sizes, step = [], 1
    while step < count:
        axis = [i for i in range(3) if spots[step][i] != spots[0][i]]
        if len(axis) != 1:
            return None
        seen = 1
        while seen * step < count and all(
            spots[seen * step][i] == spots[0][i] for i in range(3) if i != axis[0]
        ):
            seen += 1
        sizes.insert(0, seen)
        step *= seen
    return tuple(sizes)


def partner_of(at, step, size):
    return at ^ step if size & (size - 1) == 0 else (at + step) % size


def owner_at(grid, spot):
    nz, ny, nx = grid
    dz, dy, dx = spot
    me = lax.axis_index("fsdp")
    z, y, x = me // (ny * nx), me // nx % ny, me % nx
    z, y, x = partner_of(z, dz, nz), partner_of(y, dy, ny), partner_of(x, dx, nx)
    return (z * ny + y) * nx + x


def stage_kernel(grid, lists, order_hbm, x_ref, *refs):
    refs = list(refs)
    cot_ref = refs.pop(0) if len(refs) == 5 + 2 * len(lists) else None
    outs, (buf, order_ref, x_sems, sems) = refs[:-4], refs[-4:]
    chunks, step, _ = buf.shape
    half = lax.axis_index("dp") % 2
    loads = []
    for c in range(chunks):
        loads.append(
            pltpu.make_async_copy(x_ref.at[pl.ds(c * step, step)], buf.at[c], x_sems.at[c])
        )
        loads[-1].start()
    fetch = pltpu.make_async_copy(order_hbm, order_ref, sems.at[0])
    fetch.start()
    stores = []
    if cot_ref is not None:
        for k, to_ref in enumerate(outs[:2]):
            to = to_ref.at[:, len(lists[0]) * LANES :]
            stores.append(pltpu.make_async_copy(cot_ref, to, sems.at[1 + k]))
            stores[-1].start()
    fetch.wait()
    cols = [[order_ref[owner_at(grid, spot)] for spot in spots] for spots in lists]
    for c in range(chunks):
        loads[c].wait()
        rows = slice(c * step, (c + 1) * step)
        for i, to_ref in enumerate(outs):
            side = half if i % 2 == 0 else 1 - half
            for k, col in enumerate(cols[i // 2]):
                at = pl.ds(pl.multiple_of((2 * col + side) * LANES, LANES), LANES)
                to_ref[rows, k * LANES : (k + 1) * LANES] = buf[c, :, at]
    for store in stores:
        store.wait()


def wgrad_kernel(cot_at, *refs):
    sources, outs = refs[:2], refs[2:]
    cot = jnp.concatenate([r[:, cot_at:] for r in sources], axis=0)
    begin = 0
    for out in outs:
        at = slice(begin, begin + out.shape[0])
        out[...] = lax.dot_general(
            jnp.concatenate([r[:, at] for r in sources], axis=0),
            cot,
            (((0,), (0,)), ((), ())),
            preferred_element_type=jnp.float32,
        ).astype(out.dtype)
        begin += out.shape[0]


def apply_kernel(grid, pieces, first, last, order_ref, cot_ref, *refs):
    half = lax.axis_index("dp") % 2
    refs = list(refs)
    weights = [refs.pop(0) for _ in pieces]
    columns = {}
    for _, partner in pieces:
        if partner not in columns:
            columns[partner] = [refs.pop(0), 0]
    before_ref = None if first else refs.pop(0)
    if not first:
        refs.pop(0)
    halves = [refs.pop(0) for _ in range(2)] if last else []
    key_ref, grad_ref = refs.pop(0), refs.pop(0)
    buffer_ref = refs.pop(0) if last else None
    scratch, total_buf, key_buf, out_sems, sems = refs
    if not first:
        fetch = pltpu.make_async_copy(before_ref, total_buf, sems.at[0])
        fetch.start()
    stores = []
    for k, ref in enumerate(halves):
        part = ref.shape[0]
        side = half if k == 0 else 1 - half
        stores.append(
            pltpu.make_async_copy(
                ref, buffer_ref.at[pl.ds(pl.multiple_of(side * part, part), part)], sems.at[2 + k]
            )
        )
        stores[-1].start()
    cot = cot_ref[...]
    count = 0
    for place, (spots, partner) in enumerate(pieces):
        side = 1 - half if partner else half
        back = lax.dot_general(
            cot, weights[place][...], (((1,), (1,)), ((), ())), preferred_element_type=jnp.float32
        )
        scratch[place] = back.astype(scratch.dtype)
        for k, spot in enumerate(spots):
            col = order_ref[owner_at(grid, spot)]
            start = pl.multiple_of((2 * col + side) * LANES, LANES)
            stores.append(
                pltpu.make_async_copy(
                    scratch.at[place, :, k * LANES : (k + 1) * LANES],
                    grad_ref.at[:, pl.ds(start, LANES)],
                    out_sems.at[count],
                )
            )
            stores[-1].start()
            count += 1
    total = None
    for place, (spots, partner) in enumerate(pieces):
        source, begin = columns[partner]
        columns[partner][1] = end = begin + len(spots) * LANES
        term = jnp.dot(
            source[:, begin:end], weights[place][...], preferred_element_type=jnp.float32
        )
        total = term if total is None else total + term
    if not first:
        fetch.wait()
        total = total + total_buf[...]
    key_buf[...] = total.astype(key_buf.dtype)
    stores.append(pltpu.make_async_copy(key_buf, key_ref, sems.at[1]))
    stores[-1].start()
    for store in stores:
        store.wait()


def staged_body(grid, normed, kv_cotangent, kv_weight, main_grad, owner_order):
    nz, ny, nx = grid
    micro_count, tok_dev, width = normed.shape
    shard_rows, key_width = kv_weight.shape
    owners, replicas = lax.axis_size("fsdp"), lax.axis_size("dp")
    rows = micro_count * tok_dev
    part = shard_rows // 2
    half = lax.axis_index("dp") % 2
    f32, bf16 = jnp.float32, jnp.bfloat16
    vmem = pl.BlockSpec(memory_space=pltpu.VMEM)
    smem = pl.BlockSpec(memory_space=pltpu.SMEM)
    hbm = pl.BlockSpec(memory_space=pltpu.HBM)

    def send(value, move):
        pairs = []
        for z in range(nz):
            for y in range(ny):
                for x in range(nx):
                    for r in range(replicas):
                        tz, ty, tx, tr = move(z, y, x, r)
                        to = ((tz % nz) * ny + ty % ny) * nx + tx % nx
                        pairs.append((((z * ny + y) * nx + x) * replicas + r, to * replicas + tr))
        return lax.ppermute(value, ("fsdp", "dp"), pairs)

    def over_x(value):
        return send(value, lambda z, y, x, r: (z, y, partner_of(x, 1, nx), r))

    def over_y(value):
        return send(value, lambda z, y, x, r: (z, partner_of(y, 1, ny), x, r))

    def over_z(value, step):
        return send(value, lambda z, y, x, r: (partner_of(z, step, nz), y, x, r))

    def to_core(value):
        return send(value, lambda z, y, x, r: (z, y, x, r ^ 1))

    flat = normed.reshape(rows, width)
    cot = kv_cotangent.reshape(rows, key_width)
    doubling = [nz >> k for k in range(1, nz.bit_length())]
    near = [0]
    for d in doubling[:-1]:
        near = near + [d + k for k in near]
    far = [1 + k for k in near]
    red_rows, blue_rows = part * len(near), part * len(far)

    far_spots = [(k, 1, dx) for dx in (0, 1) for k in near]
    far_spots += [(k, dy, 1) for dy in (0, 1) for k in far]
    near_spots = [(k, 0, dx) for dx in (0, 1) for k in near]
    near_spots += [(k, dy, 0) for dy in (0, 1) for k in far]
    chunks = 4

    def stage(lists, extra, limit):
        shapes = []
        for spots in lists:
            wide = part * len(spots) + (extra[0].shape[1] if extra and spots is lists[0] else 0)
            shapes += [jax.ShapeDtypeStruct((rows, wide), bf16)] * 2
        return pl.pallas_call(
            functools.partial(stage_kernel, grid, lists),
            in_specs=[hbm] * (2 + len(extra)),
            out_specs=[vmem] * len(shapes),
            out_shape=shapes,
            scratch_shapes=[
                pltpu.VMEM((chunks, rows // chunks, width), bf16),
                pltpu.SMEM(owner_order.shape, jnp.int32),
                pltpu.SemaphoreType.DMA((chunks,)),
                pltpu.SemaphoreType.DMA((3,)),
            ],
            compiler_params=pltpu.CompilerParams(vmem_limit_bytes=limit),
        )(owner_order, flat, *extra)

    first_own, first_partner = stage([far_spots], [cot], TIGHT_BYTES)
    first_got = to_core(first_partner)
    near_own, near_partner, far_own, far_partner = stage([near_spots, far_spots], [cot], 8 << 20)
    near_got = to_core(near_partner)

    def wgrad(sources, sizes, dtype):
        return pl.pallas_call(
            functools.partial(wgrad_kernel, sources[0].shape[1] - key_width),
            in_specs=[vmem] * len(sources),
            out_specs=[vmem] * len(sizes),
            out_shape=[jax.ShapeDtypeStruct((size, key_width), dtype) for size in sizes],
            cost_estimate=pl.CostEstimate(
                flops=rows * width * key_width,
                bytes_accessed=4 * rows * width,
                transcendentals=0,
            ),
            compiler_params=pltpu.CompilerParams(vmem_limit_bytes=24 << 20),
        )(*sources)

    red_out, blue_out = wgrad([first_own, first_got], [2 * red_rows, 2 * blue_rows], bf16)
    red_keep, red_on, blue_keep, blue_on = wgrad(
        [near_own, near_got], [red_rows, red_rows, blue_rows, blue_rows], f32
    )

    own = lax.dynamic_slice_in_dim(kv_weight, half * part, part, axis=0)
    red = own
    for d in doubling[:-1]:
        red = jnp.concatenate([red, over_z(red, d)], axis=0)
    blue = over_z(red, 1)
    red = jnp.concatenate([red, over_x(red)], axis=0)
    blue = jnp.concatenate([blue, over_y(blue)], axis=0)
    red_y = over_y(red)
    blue_x = over_x(blue)
    red_spots, blue_spots = near_spots[: 2 * len(near)], near_spots[2 * len(near) :]
    red_y_spots, blue_x_spots = far_spots[: 2 * len(near)], far_spots[2 * len(near) :]

    red_in = over_y(red_out)
    blue_in = over_x(blue_out)
    red_far = (red_on + red_in[red_rows:]).astype(bf16)
    blue_far = (blue_on + blue_in[blue_rows:]).astype(bf16)
    red_sum = red_keep + red_in[:red_rows] + over_x(red_far)
    blue_sum = blue_keep + blue_in[:blue_rows] + over_y(blue_far)
    along = {}
    for places, sums in ((near, red_sum), (far, blue_sum)):
        for at, k in enumerate(places):
            along[k] = sums[at * part : (at + 1) * part]
    total = along[0]
    for d in range(1, nz):
        total = total + over_z(along[d].astype(bf16), d)
    if replicas > 2:
        groups = [[r for r in range(replicas) if r % 2 == h] for h in (0, 1)]
        total = lax.psum(total, "dp", axis_index_groups=groups)
    grad_scale = 1.0 / math.sqrt(rows * owners * replicas)
    kept = lax.dynamic_slice_in_dim(main_grad, half * part, part, axis=0) + total * grad_scale
    there = to_core(kept)

    def apply(pieces, columns, before, halves):
        weights = [w for w, _, _ in pieces]
        inputs = [owner_order, cot, *weights, *columns, *before, *halves]
        specs = [smem] + [vmem] * (1 + len(pieces) + len(columns)) + [hbm, hbm][: len(before)]
        specs += [vmem] * len(halves)
        count = sum(len(spots) for _, spots, _ in pieces)
        wide = max(w.shape[0] for w in weights)
        key_type = bf16 if halves else f32
        shapes = [
            jax.ShapeDtypeStruct((rows, key_width), key_type),
            jax.ShapeDtypeStruct((rows, width), bf16),
        ]
        if halves:
            shapes.append(jax.ShapeDtypeStruct((shard_rows, key_width), f32))
        return pl.pallas_call(
            functools.partial(
                apply_kernel, grid, [p[1:] for p in pieces], not before, bool(halves)
            ),
            in_specs=specs,
            out_specs=[hbm] * len(shapes),
            out_shape=shapes,
            scratch_shapes=[
                pltpu.VMEM((len(pieces), rows, wide), bf16),
                pltpu.VMEM((rows, key_width), f32),
                pltpu.VMEM((rows, key_width), key_type),
                pltpu.SemaphoreType.DMA((count,)),
                pltpu.SemaphoreType.DMA((4,)),
            ],
            input_output_aliases={len(inputs) - 1 - len(halves): 1} if before else {},
            cost_estimate=pl.CostEstimate(
                flops=4 * rows * key_width * sum(w.shape[0] for w in weights),
                bytes_accessed=2 * rows * width,
                transcendentals=0,
            ),
            compiler_params=pltpu.CompilerParams(vmem_limit_bytes=24 << 20),
        )(*inputs)

    done = apply(
        [
            (red, red_spots, False),
            (blue, blue_spots, False),
            (to_core(red), red_spots, True),
            (to_core(blue), blue_spots, True),
        ],
        [near_own, near_partner],
        (),
        (),
    )
    done = apply([(red_y, red_y_spots, False), (blue_x, blue_x_spots, False)], [far_own], done, ())
    key, input_grad, grad_buffer = apply(
        [(to_core(red_y), red_y_spots, True), (to_core(blue_x), blue_x_spots, True)],
        [far_partner],
        done,
        (kept, there),
    )
    return (
        key.reshape(micro_count, tok_dev, key_width),
        input_grad.reshape(micro_count, tok_dev, width),
        grad_buffer,
    )


def solution(mesh):
    in_specs = (
        P(None, ("fsdp", "dp"), None),
        P(None, ("fsdp", "dp"), None),
        P("fsdp", None),
        P("fsdp", None),
        P(),
    )
    out_specs = (P(None, ("fsdp", "dp"), None), P(None, ("fsdp", "dp"), None), P("fsdp", None))
    grid = grid_of(mesh)
    staged = grid is not None and len(grid) == 3 and grid[1:] == (2, 2)
    staged = staged and grid[0] & (grid[0] - 1) == 0 and grid[0] > 2
    staged = staged and mesh.shape["dp"] % 2 == 0

    def body(normed, kv_cotangent, kv_weight, main_grad, owner_order):
        args = (normed, kv_cotangent, kv_weight, main_grad, owner_order)
        if staged and kv_weight.shape[0] == 2 * LANES:
            return staged_body(grid, *args)
        return plain_body(*args)

    return jax.shard_map(body, mesh=mesh, in_specs=in_specs, out_specs=out_specs, check_vma=False)
```

```python
import functools
import math

import jax
import jax.numpy as jnp
from jax import lax
from jax.experimental import pallas as pl
from jax.experimental.pallas import tpu as pltpu
from jax.sharding import PartitionSpec as P


LANES = 128
TIGHT_BYTES = (62 << 20) + (16 << 10)


def plain_body(normed, kv_cotangent, kv_weight, main_grad, owner_order):
    micro_count, tok_dev, width = normed.shape
    shard_rows, key_width = kv_weight.shape
    owners = lax.axis_size("fsdp")
    everyone = owners * lax.axis_size("dp")
    all_rows = micro_count * tok_dev
    permuted = jnp.take(normed.reshape(all_rows, owners, shard_rows), owner_order, axis=1).reshape(
        all_rows, width
    )
    flat_cot = kv_cotangent.reshape(all_rows, key_width)
    gathered = lax.all_gather(kv_weight, "fsdp", axis=0, tiled=True)
    key_sum = jnp.dot(permuted, gathered, preferred_element_type=jnp.float32)
    grad_permuted = lax.dot_general(
        flat_cot, gathered, (((1,), (1,)), ((), ())), preferred_element_type=jnp.float32
    ).astype(jnp.bfloat16)
    inverse_owner = jnp.argsort(owner_order)
    input_grad = jnp.take(
        grad_permuted.reshape(all_rows, owners, shard_rows), inverse_owner, axis=1
    ).reshape(micro_count, tok_dev, width)
    partial = lax.dot_general(
        permuted, flat_cot, (((0,), (0,)), ((), ())), preferred_element_type=jnp.float32
    )
    shard_sum = lax.psum_scatter(partial, "fsdp", scatter_dimension=0, tiled=True)
    replica_total = lax.psum(shard_sum, "dp")
    grad_scale = 1.0 / math.sqrt(micro_count * tok_dev * everyone)
    grad_buffer = main_grad + replica_total * grad_scale
    key_rows = key_sum.astype(jnp.bfloat16).reshape(micro_count, tok_dev, key_width)
    return (key_rows, input_grad, grad_buffer)


def grid_of(mesh):
    count = mesh.shape["fsdp"]
    spots = [getattr(d, "coords", None) for d in mesh.devices.reshape(count, -1)[:, 0]]
    if any(s is None for s in spots):
        return None
    sizes, step = [], 1
    while step < count:
        axis = [i for i in range(3) if spots[step][i] != spots[0][i]]
        if len(axis) != 1:
            return None
        seen = 1
        while seen * step < count and all(
            spots[seen * step][i] == spots[0][i] for i in range(3) if i != axis[0]
        ):
            seen += 1
        sizes.insert(0, seen)
        step *= seen
    return tuple(sizes)


def partner_of(at, step, size):
    return at ^ step if size & (size - 1) == 0 else (at + step) % size


def owner_at(grid, spot, core):
    nz, ny, nx = grid
    dz, da, db = spot
    me = lax.axis_index("fsdp")
    z, y, x = me // (ny * nx), me // nx % ny, me % nx
    dy, dx = jnp.where(core == 0, da, db), jnp.where(core == 0, db, da)
    return (partner_of(z, dz, nz) * ny + (y ^ dy)) * nx + (x ^ dx)


def stage_kernel(grid, lists, order_hbm, x_ref, *refs):
    refs = list(refs)
    cot_ref = refs.pop(0) if len(refs) == 5 + 2 * len(lists) else None
    outs, (buf, order_ref, x_sems, sems) = refs[:-4], refs[-4:]
    chunks, step, _ = buf.shape
    half = lax.axis_index("dp") % 2
    loads = []
    for c in range(chunks):
        loads.append(
            pltpu.make_async_copy(x_ref.at[pl.ds(c * step, step)], buf.at[c], x_sems.at[c])
        )
        loads[-1].start()
    fetch = pltpu.make_async_copy(order_hbm, order_ref, sems.at[0])
    fetch.start()
    stores = []
    if cot_ref is not None:
        for k, to_ref in enumerate(outs[:2]):
            to = to_ref.at[:, len(lists[0]) * LANES :]
            stores.append(pltpu.make_async_copy(cot_ref, to, sems.at[1 + k]))
            stores[-1].start()
    fetch.wait()
    sides = (half, 1 - half)
    cols = [
        [order_ref[owner_at(grid, spot, side)] for spot in spots]
        for spots in lists
        for side in sides
    ]
    for c in range(chunks):
        loads[c].wait()
        rows = slice(c * step, (c + 1) * step)
        for i, to_ref in enumerate(outs):
            for k, col in enumerate(cols[i]):
                at = pl.ds(pl.multiple_of((2 * col + sides[i % 2]) * LANES, LANES), LANES)
                to_ref[rows, k * LANES : (k + 1) * LANES] = buf[c, :, at]
    for store in stores:
        store.wait()


def wgrad_kernel(cot_at, lists, *refs):
    sources, outs = refs[:2], refs[2:]
    cot = jnp.concatenate([r[:, cot_at:] for r in sources], axis=0)
    for places, out in zip(lists, outs):
        columns = [slice(p * LANES, (p + 1) * LANES) for p in places]
        both = [jnp.concatenate([r[:, c] for c in columns], axis=1) for r in sources]
        out[...] = lax.dot_general(
            jnp.concatenate(both, axis=0),
            cot,
            (((0,), (0,)), ((), ())),
            preferred_element_type=jnp.float32,
        ).astype(out.dtype)


def apply_kernel(grid, pieces, first, last, order_ref, cot_ref, *refs):
    half = lax.axis_index("dp") % 2
    refs = list(refs)
    weights = [refs.pop(0) for _ in pieces]
    columns = [refs.pop(0) for _ in range(1 + max(p[2] for p in pieces))]
    before_ref = None if first else refs.pop(0)
    if not first:
        refs.pop(0)
    halves = [refs.pop(0) for _ in range(2)] if last else []
    key_ref, grad_ref = refs.pop(0), refs.pop(0)
    buffer_ref = refs.pop(0) if last else None
    scratch, total_buf, key_buf, out_sems, sems = refs
    if not first:
        fetch = pltpu.make_async_copy(before_ref, total_buf, sems.at[0])
        fetch.start()
    stores = []
    for k, ref in enumerate(halves):
        part = ref.shape[0]
        side = half if k == 0 else 1 - half
        stores.append(
            pltpu.make_async_copy(
                ref, buffer_ref.at[pl.ds(pl.multiple_of(side * part, part), part)], sems.at[2 + k]
            )
        )
        stores[-1].start()
    cot = cot_ref[...]
    count = 0
    for place, (spots, partner, _, _) in enumerate(pieces):
        side = 1 - half if partner else half
        back = lax.dot_general(
            cot, weights[place][...], (((1,), (1,)), ((), ())), preferred_element_type=jnp.float32
        )
        scratch[place] = back.astype(scratch.dtype)
        for k, spot in enumerate(spots):
            col = order_ref[owner_at(grid, spot, side)]
            start = pl.multiple_of((2 * col + side) * LANES, LANES)
            stores.append(
                pltpu.make_async_copy(
                    scratch.at[place, :, k * LANES : (k + 1) * LANES],
                    grad_ref.at[:, pl.ds(start, LANES)],
                    out_sems.at[count],
                )
            )
            stores[-1].start()
            count += 1
    total = None
    for place, (spots, _, source, begin) in enumerate(pieces):
        source = columns[source][:, begin : begin + len(spots) * LANES]
        term = jnp.dot(source, weights[place][...], preferred_element_type=jnp.float32)
        total = term if total is None else total + term
    if not first:
        fetch.wait()
        total = total + total_buf[...]
    key_buf[...] = total.astype(key_buf.dtype)
    stores.append(pltpu.make_async_copy(key_buf, key_ref, sems.at[1]))
    stores[-1].start()
    for store in stores:
        store.wait()


def staged_body(grid, normed, kv_cotangent, kv_weight, main_grad, owner_order):
    nz, ny, nx = grid
    micro_count, tok_dev, width = normed.shape
    shard_rows, key_width = kv_weight.shape
    owners, replicas = lax.axis_size("fsdp"), lax.axis_size("dp")
    rows = micro_count * tok_dev
    part = shard_rows // 2
    half = lax.axis_index("dp") % 2
    f32, bf16 = jnp.float32, jnp.bfloat16
    vmem = pl.BlockSpec(memory_space=pltpu.VMEM)
    smem = pl.BlockSpec(memory_space=pltpu.SMEM)
    hbm = pl.BlockSpec(memory_space=pltpu.HBM)

    def send(value, move):
        pairs = []
        for z in range(nz):
            for y in range(ny):
                for x in range(nx):
                    for r in range(replicas):
                        tz, ty, tx, tr = move(z, y, x, r)
                        to = ((tz % nz) * ny + ty % ny) * nx + tx % nx
                        pairs.append((((z * ny + y) * nx + x) * replicas + r, to * replicas + tr))
        return lax.ppermute(value, ("fsdp", "dp"), pairs)

    def over_first(value):
        return send(value, lambda z, y, x, r: (z, y, x ^ 1, r) if r % 2 else (z, y ^ 1, x, r))

    def over_second(value):
        return send(value, lambda z, y, x, r: (z, y ^ 1, x, r) if r % 2 else (z, y, x ^ 1, r))

    def over_z(value, step):
        return send(value, lambda z, y, x, r: (partner_of(z, step, nz), y, x, r))

    def to_core(value):
        return send(value, lambda z, y, x, r: (z, y, x, r ^ 1))

    flat = normed.reshape(rows, width)
    cot = kv_cotangent.reshape(rows, key_width)
    doubling = [nz >> k for k in range(1, nz.bit_length())]
    line = [0]
    for d in doubling:
        line = line + [d + k for k in line]
    line_rows = part * nz
    groups = [[k for k in line if k >= nz // 2], [k for k in line if k < nz // 2]]
    group_rows = line_rows // 2

    near_spots, far_spots = ([(k, da, db) for db in (0, 1) for k in line] for da in (0, 1))
    chunks = 4

    def stage(lists, extra, limit):
        shapes = []
        for spots in lists:
            wide = part * len(spots) + (extra[0].shape[1] if extra and spots is lists[0] else 0)
            shapes += [jax.ShapeDtypeStruct((rows, wide), bf16)] * 2
        return pl.pallas_call(
            functools.partial(stage_kernel, grid, lists),
            in_specs=[hbm] * (2 + len(extra)),
            out_specs=[vmem] * len(shapes),
            out_shape=shapes,
            scratch_shapes=[
                pltpu.VMEM((chunks, rows // chunks, width), bf16),
                pltpu.SMEM(owner_order.shape, jnp.int32),
                pltpu.SemaphoreType.DMA((chunks,)),
                pltpu.SemaphoreType.DMA((3,)),
            ],
            compiler_params=pltpu.CompilerParams(vmem_limit_bytes=limit),
        )(owner_order, flat, *extra)

    first_spots = [(k, 1, db) for ks in groups for db in (0, 1) for k in ks]
    first_own, first_partner = stage([first_spots], [cot], TIGHT_BYTES)
    first_got = to_core(first_partner)
    near_own, near_partner, far_own, far_partner = stage([near_spots, far_spots], [cot], 8 << 20)
    near_got = to_core(near_partner)

    def wgrad(sources, order, lists, dtype):
        places = [[order.index(spot) for spot in spots] for spots in lists]
        cot_at = sources[0].shape[1] - key_width
        return pl.pallas_call(
            functools.partial(wgrad_kernel, cot_at, places),
            in_specs=[vmem] * 2,
            out_specs=[vmem] * len(lists),
            out_shape=[
                jax.ShapeDtypeStruct((part * len(s), key_width), dtype) for s in lists
            ],
            cost_estimate=pl.CostEstimate(
                flops=rows * width * key_width,
                bytes_accessed=4 * rows * width,
                transcendentals=0,
            ),
            compiler_params=pltpu.CompilerParams(vmem_limit_bytes=24 << 20),
        )(*sources)

    outs = wgrad(
        [first_own, first_got],
        first_spots,
        [[(k, 1, db) for db in (0, 1) for k in ks] for ks in groups],
        bf16,
    )
    kept_terms = wgrad(
        [near_own, near_got],
        near_spots,
        [[(k, 0, db) for k in ks] for ks in groups for db in (0, 1)],
        f32,
    )

    held = lax.dynamic_slice_in_dim(kv_weight, half * part, part, axis=0)
    for d in doubling:
        held = jnp.concatenate([held, over_z(held, d)], axis=0)
    beside = over_first(held)
    across = over_second(held)
    corner = over_second(beside)

    along = {}
    for i, ks in enumerate(groups):
        keep, on = kept_terms[2 * i : 2 * i + 2]
        arrived = over_first(outs[i])
        onward = (on + arrived[group_rows:]).astype(bf16)
        last = over_second(onward)
        sums = keep + arrived[:group_rows] + last
        for at, k in enumerate(ks):
            piece = sums[at * part : (at + 1) * part]
            along[k] = piece.astype(bf16) if k else piece
    total = along[0]
    for d in range(nz - 1, 0, -1):
        total = total + over_z(along[d], d)
    if replicas > 2:
        groups = [[r for r in range(replicas) if r % 2 == h] for h in (0, 1)]
        total = lax.psum(total, "dp", axis_index_groups=groups)
    grad_scale = 1.0 / math.sqrt(rows * owners * replicas)
    kept = lax.dynamic_slice_in_dim(main_grad, half * part, part, axis=0) + total * grad_scale
    there = to_core(kept)

    def apply(pieces, columns, before, halves):
        weights = [p[0] for p in pieces]
        inputs = [owner_order, cot, *weights, *columns, *before, *halves]
        specs = [smem] + [vmem] * (1 + len(pieces) + len(columns)) + [hbm, hbm][: len(before)]
        specs += [vmem] * len(halves)
        count = sum(len(p[1]) for p in pieces)
        wide = max(w.shape[0] for w in weights)
        key_type = bf16 if halves else f32
        shapes = [
            jax.ShapeDtypeStruct((rows, key_width), key_type),
            jax.ShapeDtypeStruct((rows, width), bf16),
        ]
        if halves:
            shapes.append(jax.ShapeDtypeStruct((shard_rows, key_width), f32))
        return pl.pallas_call(
            functools.partial(
                apply_kernel, grid, [p[1:] for p in pieces], not before, bool(halves)
            ),
            in_specs=specs,
            out_specs=[hbm] * len(shapes),
            out_shape=shapes,
            scratch_shapes=[
                pltpu.VMEM((len(pieces), rows, wide), bf16),
                pltpu.VMEM((rows, key_width), f32),
                pltpu.VMEM((rows, key_width), key_type),
                pltpu.SemaphoreType.DMA((count,)),
                pltpu.SemaphoreType.DMA((4,)),
            ],
            input_output_aliases={len(inputs) - 1 - len(halves): 1} if before else {},
            cost_estimate=pl.CostEstimate(
                flops=4 * rows * key_width * sum(w.shape[0] for w in weights),
                bytes_accessed=2 * rows * width,
                transcendentals=0,
            ),
            compiler_params=pltpu.CompilerParams(vmem_limit_bytes=24 << 20),
        )(*inputs)

    spots = {(da, db): [(k, da, db) for k in line] for da in (0, 1) for db in (0, 1)}
    done = apply(
        [
            (held, spots[0, 0], False, 0, 0),
            (beside, spots[1, 0], False, 1, 0),
            (to_core(held), spots[0, 0], True, 2, 0),
            (to_core(beside), spots[1, 0], True, 3, 0),
        ],
        [near_own, far_own, near_partner, far_partner],
        (),
        (),
    )
    done = apply(
        [
            (across, spots[0, 1], False, 0, line_rows),
            (to_core(across), spots[0, 1], True, 1, line_rows),
        ],
        [near_own, near_partner],
        done,
        (),
    )
    done = apply([(corner, spots[1, 1], False, 0, line_rows)], [far_own], done, ())
    key, input_grad, grad_buffer = apply(
        [(to_core(corner), spots[1, 1], True, 0, line_rows)], [far_partner], done, (kept, there)
    )
    return (
        key.reshape(micro_count, tok_dev, key_width),
        input_grad.reshape(micro_count, tok_dev, width),
        grad_buffer,
    )


def solution(mesh):
    in_specs = (
        P(None, ("fsdp", "dp"), None),
        P(None, ("fsdp", "dp"), None),
        P("fsdp", None),
        P("fsdp", None),
        P(),
    )
    out_specs = (P(None, ("fsdp", "dp"), None), P(None, ("fsdp", "dp"), None), P("fsdp", None))
    grid = grid_of(mesh)
    staged = grid is not None and len(grid) == 3 and grid[1:] == (2, 2)
    staged = staged and grid[0] & (grid[0] - 1) == 0 and grid[0] > 2
    staged = staged and mesh.shape["dp"] % 2 == 0

    def body(normed, kv_cotangent, kv_weight, main_grad, owner_order):
        args = (normed, kv_cotangent, kv_weight, main_grad, owner_order)
        if staged and kv_weight.shape[0] == 2 * LANES:
            return staged_body(grid, *args)
        return plain_body(*args)

    return jax.shard_map(body, mesh=mesh, in_specs=in_specs, out_specs=out_specs, check_vma=False)
```

```python
import functools
import math

import jax
import jax.numpy as jnp
from jax import lax
from jax.experimental import pallas as pl
from jax.experimental.pallas import tpu as pltpu
from jax.sharding import PartitionSpec as P


LANES = 128
TIGHT_BYTES = (62 << 20) + (16 << 10)


def plain_body(normed, kv_cotangent, kv_weight, main_grad, owner_order):
    micro_count, tok_dev, width = normed.shape
    shard_rows, key_width = kv_weight.shape
    owners = lax.axis_size("fsdp")
    everyone = owners * lax.axis_size("dp")
    all_rows = micro_count * tok_dev
    permuted = jnp.take(normed.reshape(all_rows, owners, shard_rows), owner_order, axis=1).reshape(
        all_rows, width
    )
    flat_cot = kv_cotangent.reshape(all_rows, key_width)
    gathered = lax.all_gather(kv_weight, "fsdp", axis=0, tiled=True)
    key_sum = jnp.dot(permuted, gathered, preferred_element_type=jnp.float32)
    grad_permuted = lax.dot_general(
        flat_cot, gathered, (((1,), (1,)), ((), ())), preferred_element_type=jnp.float32
    ).astype(jnp.bfloat16)
    inverse_owner = jnp.argsort(owner_order)
    input_grad = jnp.take(
        grad_permuted.reshape(all_rows, owners, shard_rows), inverse_owner, axis=1
    ).reshape(micro_count, tok_dev, width)
    partial = lax.dot_general(
        permuted, flat_cot, (((0,), (0,)), ((), ())), preferred_element_type=jnp.float32
    )
    shard_sum = lax.psum_scatter(partial, "fsdp", scatter_dimension=0, tiled=True)
    replica_total = lax.psum(shard_sum, "dp")
    grad_scale = 1.0 / math.sqrt(micro_count * tok_dev * everyone)
    grad_buffer = main_grad + replica_total * grad_scale
    key_rows = key_sum.astype(jnp.bfloat16).reshape(micro_count, tok_dev, key_width)
    return (key_rows, input_grad, grad_buffer)


def grid_of(mesh):
    count = mesh.shape["fsdp"]
    spots = [getattr(d, "coords", None) for d in mesh.devices.reshape(count, -1)[:, 0]]
    if any(s is None for s in spots):
        return None
    sizes, step = [], 1
    while step < count:
        axis = [i for i in range(3) if spots[step][i] != spots[0][i]]
        if len(axis) != 1:
            return None
        seen = 1
        while seen * step < count and all(
            spots[seen * step][i] == spots[0][i] for i in range(3) if i != axis[0]
        ):
            seen += 1
        sizes.insert(0, seen)
        step *= seen
    return tuple(sizes)


def partner_of(at, step, size):
    return at ^ step if size & (size - 1) == 0 else (at + step) % size


def owner_at(grid, spot, core):
    nz, ny, nx = grid
    dz, da, db = spot
    me = lax.axis_index("fsdp")
    z, y, x = me // (ny * nx), me // nx % ny, me % nx
    dy, dx = jnp.where(core == 0, da, db), jnp.where(core == 0, db, da)
    return (partner_of(z, dz, nz) * ny + (y ^ dy)) * nx + (x ^ dx)


def stage_kernel(grid, lists, direct, order_hbm, x_ref, *refs):
    count = 2 * len(lists)
    cot_ref, outs, refs = refs[0], refs[1 : 1 + count], refs[1 + count :]
    laid = outs if direct else refs[:count]
    buf, order_ref, x_sems, out_sems, sems = refs[-5:]
    chunks, step, _ = buf.shape
    half = lax.axis_index("dp") % 2
    loads = []
    for c in range(chunks):
        loads.append(
            pltpu.make_async_copy(x_ref.at[pl.ds(c * step, step)], buf.at[c], x_sems.at[c])
        )
        loads[-1].start()
    fetch = pltpu.make_async_copy(order_hbm, order_ref, sems.at[0])
    fetch.start()
    cots = []
    for i, to_ref in enumerate(laid):
        wide = LANES * len(lists[i // 2])
        if to_ref.shape[1] > wide:
            to = to_ref.at[:, wide:]
            cots.append(pltpu.make_async_copy(cot_ref, to, sems.at[1 + len(cots)]))
            cots[-1].start()
    fetch.wait()
    sides = (half, 1 - half)
    cols = [
        [order_ref[owner_at(grid, spot, side)] for spot in spots]
        for spots in lists
        for side in sides
    ]
    for copy in cots:
        copy.wait()
    stores = []
    for c in range(chunks):
        loads[c].wait()
        rows = slice(c * step, (c + 1) * step)
        for i, to_ref in enumerate(laid):
            for k, col in enumerate(cols[i]):
                at = pl.ds(pl.multiple_of((2 * col + sides[i % 2]) * LANES, LANES), LANES)
                to_ref[rows, k * LANES : (k + 1) * LANES] = buf[c, :, at]
            if not direct:
                sem = out_sems.at[c * count + i]
                stores.append(pltpu.make_async_copy(to_ref.at[rows], outs[i].at[rows], sem))
                stores[-1].start()
    for store in stores:
        store.wait()


def wgrad_kernel(cot_at, lists, *refs):
    sources, outs = refs[:2], refs[2:]
    cot = jnp.concatenate([r[:, cot_at:] for r in sources], axis=0)
    for places, out in zip(lists, outs):
        columns = [slice(p * LANES, (p + 1) * LANES) for p in places]
        both = [jnp.concatenate([r[:, c] for c in columns], axis=1) for r in sources]
        out[...] = lax.dot_general(
            jnp.concatenate(both, axis=0),
            cot,
            (((0,), (0,)), ((), ())),
            preferred_element_type=jnp.float32,
        ).astype(out.dtype)


def apply_kernel(grid, pieces, first, last, order_ref, cot_ref, *refs):
    half = lax.axis_index("dp") % 2
    refs = list(refs)
    weights = [refs.pop(0) for _ in pieces]
    columns = [refs.pop(0) for _ in range(1 + max(p[2] for p in pieces))]
    before_ref = None if first else refs.pop(0)
    if not first:
        refs.pop(0)
    halves = [refs.pop(0) for _ in range(2)] if last else []
    key_ref, grad_ref = refs.pop(0), refs.pop(0)
    buffer_ref = refs.pop(0) if last else None
    scratch, total_buf, key_buf, out_sems, sems = refs
    if not first:
        fetch = pltpu.make_async_copy(before_ref, total_buf, sems.at[0])
        fetch.start()
    stores = []
    for k, ref in enumerate(halves):
        part = ref.shape[0]
        side = half if k == 0 else 1 - half
        stores.append(
            pltpu.make_async_copy(
                ref, buffer_ref.at[pl.ds(pl.multiple_of(side * part, part), part)], sems.at[2 + k]
            )
        )
        stores[-1].start()
    cot = cot_ref[...]
    count = 0
    for place, (spots, partner, _, _) in enumerate(pieces):
        side = 1 - half if partner else half
        back = lax.dot_general(
            cot, weights[place][...], (((1,), (1,)), ((), ())), preferred_element_type=jnp.float32
        )
        scratch[place] = back.astype(scratch.dtype)
        for k, spot in enumerate(spots):
            col = order_ref[owner_at(grid, spot, side)]
            start = pl.multiple_of((2 * col + side) * LANES, LANES)
            stores.append(
                pltpu.make_async_copy(
                    scratch.at[place, :, k * LANES : (k + 1) * LANES],
                    grad_ref.at[:, pl.ds(start, LANES)],
                    out_sems.at[count],
                )
            )
            stores[-1].start()
            count += 1
    total = None
    for place, (spots, _, source, begin) in enumerate(pieces):
        source = columns[source][:, begin : begin + len(spots) * LANES]
        term = jnp.dot(source, weights[place][...], preferred_element_type=jnp.float32)
        total = term if total is None else total + term
    if not first:
        fetch.wait()
        total = total + total_buf[...]
    key_buf[...] = total.astype(key_buf.dtype)
    stores.append(pltpu.make_async_copy(key_buf, key_ref, sems.at[1]))
    stores[-1].start()
    for store in stores:
        store.wait()


def staged_body(grid, normed, kv_cotangent, kv_weight, main_grad, owner_order):
    nz, ny, nx = grid
    micro_count, tok_dev, width = normed.shape
    shard_rows, key_width = kv_weight.shape
    owners, replicas = lax.axis_size("fsdp"), lax.axis_size("dp")
    rows = micro_count * tok_dev
    part = shard_rows // 2
    half = lax.axis_index("dp") % 2
    f32, bf16 = jnp.float32, jnp.bfloat16
    vmem = pl.BlockSpec(memory_space=pltpu.VMEM)
    smem = pl.BlockSpec(memory_space=pltpu.SMEM)
    hbm = pl.BlockSpec(memory_space=pltpu.HBM)

    def send(value, move):
        pairs = []
        for z in range(nz):
            for y in range(ny):
                for x in range(nx):
                    for r in range(replicas):
                        tz, ty, tx, tr = move(z, y, x, r)
                        to = ((tz % nz) * ny + ty % ny) * nx + tx % nx
                        pairs.append((((z * ny + y) * nx + x) * replicas + r, to * replicas + tr))
        return lax.ppermute(value, ("fsdp", "dp"), pairs)

    def over_first(value):
        return send(value, lambda z, y, x, r: (z, y, x ^ 1, r) if r % 2 else (z, y ^ 1, x, r))

    def over_second(value):
        return send(value, lambda z, y, x, r: (z, y ^ 1, x, r) if r % 2 else (z, y, x ^ 1, r))

    def over_z(value, step):
        return send(value, lambda z, y, x, r: (partner_of(z, step, nz), y, x, r))

    def to_core(value):
        return send(value, lambda z, y, x, r: (z, y, x, r ^ 1))

    flat = normed.reshape(rows, width)
    cot = kv_cotangent.reshape(rows, key_width)
    doubling = [nz >> k for k in range(1, nz.bit_length())]
    line = [0]
    for d in doubling:
        line = line + [d + k for k in line]
    line_rows = part * nz
    groups = [[k for k in line if k >= nz // 2], [k for k in line if k < nz // 2]]
    group_rows = line_rows // 2

    near_spots, far_spots = ([(k, da, db) for db in (0, 1) for k in line] for da in (0, 1))
    chunks = 4

    def stage(lists, given, direct, limit):
        shapes = []
        for i in range(2 * len(lists)):
            wide = part * len(lists[i // 2]) + (key_width if i in given else 0)
            shapes.append(jax.ShapeDtypeStruct((rows, wide), bf16))
        return pl.pallas_call(
            functools.partial(stage_kernel, grid, lists, direct),
            in_specs=[hbm] * 3,
            out_specs=[vmem if direct else hbm] * len(shapes),
            out_shape=shapes,
            scratch_shapes=[pltpu.VMEM(s.shape, bf16) for s in shapes if not direct]
            + [
                pltpu.VMEM((chunks, rows // chunks, width), bf16),
                pltpu.SMEM(owner_order.shape, jnp.int32),
                pltpu.SemaphoreType.DMA((chunks,)),
                pltpu.SemaphoreType.DMA((chunks * len(shapes),)),
                pltpu.SemaphoreType.DMA((3,)),
            ],
            compiler_params=pltpu.CompilerParams(vmem_limit_bytes=limit),
        )(owner_order, flat, cot)

    first_spots = [(k, 1, db) for ks in groups for db in (0, 1) for k in ks]
    first_own, first_partner = stage([first_spots], (1,), False, TIGHT_BYTES)
    first_own = jnp.concatenate([first_own, cot], axis=1)
    first_got = to_core(first_partner)
    near_own, near_partner, far_own, far_partner = stage(
        [near_spots, far_spots], (0, 1), True, 8 << 20
    )
    near_got = to_core(near_partner)

    def wgrad(sources, order, lists, dtype):
        places = [[order.index(spot) for spot in spots] for spots in lists]
        cot_at = sources[0].shape[1] - key_width
        return pl.pallas_call(
            functools.partial(wgrad_kernel, cot_at, places),
            in_specs=[vmem] * 2,
            out_specs=[vmem] * len(lists),
            out_shape=[
                jax.ShapeDtypeStruct((part * len(s), key_width), dtype) for s in lists
            ],
            cost_estimate=pl.CostEstimate(
                flops=rows * width * key_width,
                bytes_accessed=4 * rows * width,
                transcendentals=0,
            ),
            compiler_params=pltpu.CompilerParams(vmem_limit_bytes=24 << 20),
        )(*sources)

    outs = wgrad(
        [first_own, first_got],
        first_spots,
        [[(k, 1, db) for db in (0, 1) for k in ks] for ks in groups],
        bf16,
    )
    kept_terms = wgrad(
        [near_own, near_got],
        near_spots,
        [[(k, 0, db) for k in ks] for ks in groups for db in (0, 1)],
        f32,
    )

    def gather_z(value):
        for d in doubling:
            value = jnp.concatenate([value, over_z(value, d)], axis=0)
        return value

    own = lax.dynamic_slice_in_dim(kv_weight, half * part, part, axis=0)
    held = gather_z(own)
    beside = gather_z(over_first(own))
    across = over_second(held)
    corner = over_second(beside)

    along = {}
    for i, ks in enumerate(groups):
        keep, on = kept_terms[2 * i : 2 * i + 2]
        arrived = over_first(outs[i])
        onward = (on + arrived[group_rows:]).astype(bf16)
        last = over_second(onward)
        sums = keep + arrived[:group_rows] + last
        for at, k in enumerate(ks):
            piece = sums[at * part : (at + 1) * part]
            along[k] = piece.astype(bf16) if k else piece
    total = along[0]
    for d in range(nz - 1, 0, -1):
        total = total + over_z(along[d], d)
    if replicas > 2:
        groups = [[r for r in range(replicas) if r % 2 == h] for h in (0, 1)]
        total = lax.psum(total, "dp", axis_index_groups=groups)
    grad_scale = 1.0 / math.sqrt(rows * owners * replicas)
    kept = lax.dynamic_slice_in_dim(main_grad, half * part, part, axis=0) + total * grad_scale
    there = to_core(kept)

    def apply(pieces, columns, before, halves):
        weights = [p[0] for p in pieces]
        inputs = [owner_order, cot, *weights, *columns, *before, *halves]
        specs = [smem] + [vmem] * (1 + len(pieces) + len(columns)) + [hbm, hbm][: len(before)]
        specs += [vmem] * len(halves)
        count = sum(len(p[1]) for p in pieces)
        wide = max(w.shape[0] for w in weights)
        key_type = bf16 if halves else f32
        shapes = [
            jax.ShapeDtypeStruct((rows, key_width), key_type),
            jax.ShapeDtypeStruct((rows, width), bf16),
        ]
        if halves:
            shapes.append(jax.ShapeDtypeStruct((shard_rows, key_width), f32))
        return pl.pallas_call(
            functools.partial(
                apply_kernel, grid, [p[1:] for p in pieces], not before, bool(halves)
            ),
            in_specs=specs,
            out_specs=[hbm] * len(shapes),
            out_shape=shapes,
            scratch_shapes=[
                pltpu.VMEM((len(pieces), rows, wide), bf16),
                pltpu.VMEM((rows, key_width), f32),
                pltpu.VMEM((rows, key_width), key_type),
                pltpu.SemaphoreType.DMA((count,)),
                pltpu.SemaphoreType.DMA((4,)),
            ],
            input_output_aliases={len(inputs) - 1 - len(halves): 1} if before else {},
            cost_estimate=pl.CostEstimate(
                flops=4 * rows * key_width * sum(w.shape[0] for w in weights),
                bytes_accessed=2 * rows * width,
                transcendentals=0,
            ),
            compiler_params=pltpu.CompilerParams(vmem_limit_bytes=24 << 20),
        )(*inputs)

    spots = {(da, db): [(k, da, db) for k in line] for da in (0, 1) for db in (0, 1)}
    done = apply(
        [
            (held, spots[0, 0], False, 0, 0),
            (to_core(held), spots[0, 0], True, 1, 0),
        ],
        [near_own, near_partner],
        (),
        (),
    )
    done = apply(
        [
            (beside, spots[1, 0], False, 0, 0),
            (to_core(beside), spots[1, 0], True, 1, 0),
        ],
        [far_own, far_partner],
        done,
        (),
    )
    done = apply(
        [
            (across, spots[0, 1], False, 0, line_rows),
            (to_core(across), spots[0, 1], True, 1, line_rows),
        ],
        [near_own, near_partner],
        done,
        (),
    )
    done = apply([(corner, spots[1, 1], False, 0, line_rows)], [far_own], done, ())
    key, input_grad, grad_buffer = apply(
        [(to_core(corner), spots[1, 1], True, 0, line_rows)], [far_partner], done, (kept, there)
    )
    return (
        key.reshape(micro_count, tok_dev, key_width),
        input_grad.reshape(micro_count, tok_dev, width),
        grad_buffer,
    )


def solution(mesh):
    in_specs = (
        P(None, ("fsdp", "dp"), None),
        P(None, ("fsdp", "dp"), None),
        P("fsdp", None),
        P("fsdp", None),
        P(),
    )
    out_specs = (P(None, ("fsdp", "dp"), None), P(None, ("fsdp", "dp"), None), P("fsdp", None))
    grid = grid_of(mesh)
    staged = grid is not None and len(grid) == 3 and grid[1:] == (2, 2)
    staged = staged and grid[0] & (grid[0] - 1) == 0 and grid[0] > 2
    staged = staged and mesh.shape["dp"] % 2 == 0

    def body(normed, kv_cotangent, kv_weight, main_grad, owner_order):
        args = (normed, kv_cotangent, kv_weight, main_grad, owner_order)
        if staged and kv_weight.shape[0] == 2 * LANES:
            return staged_body(grid, *args)
        return plain_body(*args)

    return jax.shard_map(body, mesh=mesh, in_specs=in_specs, out_specs=out_specs, check_vma=False)
```
